32 devices in a mesh: row: 4 (over x, core), col: 4 (over z), depth: 2 (over y).
Axes of the slice: x: 2, y: 2, z: 4, core: 2. Of those that a mesh axis runs over, the one named last changes fastest.
Arguments:
- trailing: float32 [3008, 48128], P('depth', ('row', 'col')), may hold values from -6 to 6
- panel_block: float32 [48128, 1024], P(('row', 'col', 'depth')), may hold values from -6 to 6
- factor_panel: float32 [48128, 1024], P(('row', 'col', 'depth')), may hold values from -0.1875 to 0.1875
- corner_block: float32 [1024, 1024], P(('row', 'col', 'depth')), may hold values from -6 to 6, as said below
- corner_inverse: float32 [1024, 1024], P(('row', 'col', 'depth')), may hold values from -1 to 2, as said below
Outputs:
- trailing_out: float32 [3008, 48128], P('depth', ('row', 'col'))
- panel_out: float32 [48128, 1024], P(('row', 'col', 'depth'))
- corner_out: float32 [1024, 1024], P(('row', 'col', 'depth'))
The draws below stay inside these ranges and needn't reach their ends.
Inputs may be any that keep to these rules, and one draw needn't show every extreme that they name: `corner_block`: symmetric. `corner_inverse`: lower triangular, diagonal between 1 and 2.
All inputs are finite; a program needn't handle non-finite values.
Results may differ from the reference program's by a relative error of at most 0.00012.
Values sent between devices are 32-bit elements; how exact they have to be, the bound alone decides.
A program may use at most 192 MiB of HBM per device.

```python
import jax
import jax.numpy as jnp
from jax import lax

NB = 1024
M = 48128
SPAN = 1
SLAB = 3008
N_DEPTH = 2


def draw_corner_block(key, part):
    noise = jax.random.truncated_normal(jax.random.fold_in(key, 11), -4.0, 4.0, (NB, NB), jnp.float32)
    return (noise + noise.T) * 0.7071


def draw_corner_inverse(key, part):
    below = jax.random.truncated_normal(jax.random.fold_in(key, 23), -4.0, 4.0, (NB, NB), jnp.float32)
    diagonal = jax.random.uniform(jax.random.fold_in(key, 29), (NB,), jnp.float32, 1.0, 2.0)
    strict = jnp.tril(below, -1) * (0.5 / NB ** 0.5)
    return strict + jnp.diag(diagonal)


def block_scale(rng, shape, cuts, least, largest):
    level = 1.0
    for position, shards_of in cuts:
        draws = jax.random.uniform(jax.random.fold_in(jax.random.fold_in(rng, 6), position), (shards_of,), jnp.float32, least / len(cuts), largest / len(cuts))
        level = level * jnp.repeat(jnp.exp(draws), shape[position] // shards_of).reshape((-1,) + (1,) * (len(shape) - 1 - position))
    return level


def gaussian(stream_key, shape, scale, limit, cuts=(), dtype=jnp.bfloat16):
    loudness = block_scale(stream_key, shape, cuts, -0.22, 0.18) if cuts else 1.0
    array = jax.random.normal(stream_key, shape, jnp.float32) * scale * loudness
    return jnp.minimum(jnp.maximum(array, -limit), limit).astype(dtype)


def setup_inputs(seed: int = 0) -> dict:
    arg_keys = jax.random.split(jax.random.key(seed), 6)
    trailing = gaussian(arg_keys[0], (SLAB, M), 1.0, 6.0, ((0, 2), (1, 16)), jnp.float32)
    panel_block = gaussian(arg_keys[1], (M, NB), 1.0, 6.0, ((0, 32),), jnp.float32)
    factor_panel = gaussian(arg_keys[2], (M, NB), NB ** -0.5, 0.1875, ((0, 32),), jnp.float32)
    corner_block = draw_corner_block(jax.random.fold_in(arg_keys[5], 71), 0)
    corner_inverse = draw_corner_inverse(jax.random.fold_in(arg_keys[5], 71), 0)
    return dict(trailing=trailing, panel_block=panel_block, factor_panel=factor_panel, corner_block=corner_block, corner_inverse=corner_inverse)


def matmul(left, right):
    return jnp.dot(left, right, precision=lax.Precision.HIGHEST, preferred_element_type=jnp.float32)


def permute(matrix):
    block = matrix[:SLAB]
    shaped = block.reshape(SPAN, N_DEPTH, SLAB // (SPAN * N_DEPTH), block.shape[1])
    return jnp.transpose(shaped, (1, 0, 2, 3)).reshape(SLAB, block.shape[1])


def reference(trailing, panel_block, factor_panel, corner_block, corner_inverse):
    corner_out = matmul(corner_inverse, matmul(corner_block, corner_inverse.T))
    scaled = matmul(panel_block, corner_inverse.T)
    coupling = matmul(factor_panel, corner_out)
    half_panel = scaled - 0.5 * coupling
    panel_out = half_panel - 0.5 * coupling
    update = matmul(permute(half_panel), factor_panel.T) + matmul(permute(factor_panel), half_panel.T)
    trailing_out = trailing - update
    return trailing_out, panel_out, corner_out
```

```python
import jax
import jax.numpy as jnp
from jax import lax
from jax.sharding import PartitionSpec as P

EVERY = ("row", "col", "depth")
PIECES = 1


def matmul(left, right):
    return jnp.dot(left, right, precision=lax.Precision.HIGH, preferred_element_type=jnp.float32)


def contract(left, right):
    return lax.dot_general(
        left,
        right,
        (((1,), (1,)), ((), ())),
        precision=lax.Precision.HIGH,
        preferred_element_type=jnp.float32,
    )


def after(value, earlier):
    return lax.optimization_barrier((value, earlier))[0]


def gather_corner(corner_block, corner_inverse):
    rows, width = corner_inverse.shape
    first = lax.axis_index(EVERY) * rows
    row = first + lax.broadcasted_iota(jnp.int32, (rows, width), 0)
    col = lax.broadcasted_iota(jnp.int32, (rows, width), 1)
    both = jnp.where(col > row, corner_block, corner_inverse)
    diagonal = jnp.sum(jnp.where(col == row, corner_block, 0.0), axis=1, keepdims=True)
    packed = jnp.concatenate([both, jnp.broadcast_to(diagonal, (rows, 128))], axis=1)
    return lax.all_gather(packed, EVERY, axis=0, tiled=True)


def unpack_corner(packed, width):
    row = lax.broadcasted_iota(jnp.int32, (width, width), 0)
    col = lax.broadcasted_iota(jnp.int32, (width, width), 1)
    both = packed[:, :width]
    inverse = jnp.where(col <= row, both, 0.0)
    upper = jnp.where(col > row, both, jnp.where(col == row, 0.5 * packed[:, width:width + 1], 0.0))
    return inverse, upper


def transform(panel, factor, inverse, corner):
    coupling = matmul(factor, corner)
    half = contract(panel, inverse) - 0.5 * coupling
    return half - 0.5 * coupling


def exchange(value, layers):
    blocks = [value]
    for shift in range(1, layers):
        pairs = [(source, (source + shift) % layers) for source in range(layers)]
        blocks.append(lax.ppermute(value, "depth", pairs))
    return blocks


def arrange(blocks, layers):
    if layers == 1:
        return blocks[0]
    me = lax.axis_index("depth")
    rows, width = blocks[0].shape
    whole = jnp.zeros((layers * rows, width), blocks[0].dtype)
    for shift, block in enumerate(blocks):
        place = lax.rem(me - shift + layers, layers)
        whole = lax.dynamic_update_slice(whole, block, (place * rows, 0))
    return whole


def make_body(layers):
    def body(trailing, panel_block, factor_panel, corner_block, corner_inverse):
        rows, width = panel_block.shape
        factor_blocks = exchange(factor_panel, layers)
        panel_blocks = exchange(panel_block, layers)
        packed = gather_corner(corner_block, corner_inverse)

        count = PIECES if rows % PIECES == 0 else 1
        size = rows // count
        source = lax.axis_index(("row", "col")) == 0
        slabs = []
        for piece in range(count):
            part = slice(piece * size, (piece + 1) * size)
            pair = (panel_block[part], factor_panel[part])
            if piece:
                pair = after(pair, slabs[-1])
            kept = jnp.where(source, jnp.concatenate(pair, axis=0), 0.0)
            slabs.append(lax.psum(kept, ("row", "col")))

        inverse, upper = unpack_corner(packed, width)
        triangle = matmul(inverse, contract(upper, inverse))
        corner = triangle + triangle.T
        corner_rows = corner_inverse.shape[0]
        corner_out = lax.dynamic_slice(
            corner, (lax.axis_index(EVERY) * corner_rows, 0), (corner_rows, width)
        )
        panel_out = transform(panel_block, factor_panel, inverse, corner)

        factor_cols = arrange(factor_blocks, layers)
        panel_cols = arrange(panel_blocks, layers)
        outs = []
        for piece in range(count):
            panel_piece, factor_piece = slabs[piece][:size], slabs[piece][size:]
            left = transform(panel_piece, factor_piece, inverse, corner)
            right = matmul(factor_piece, inverse)
            part = trailing[piece * size:(piece + 1) * size]
            outs.append((part - contract(left, factor_cols)) - contract(right, panel_cols))
        trailing_out = jnp.concatenate(outs, axis=0)
        return (trailing_out, panel_out, corner_out)

    return body


def solution(mesh):
    in_specs = (
        P("depth", ("row", "col")),
        P(EVERY, None),
        P(EVERY, None),
        P(EVERY, None),
        P(EVERY, None),
    )
    out_specs = (
        P("depth", ("row", "col")),
        P(EVERY, None),
        P(EVERY, None),
    )
    body = make_body(mesh.shape["depth"])
    return jax.shard_map(body, mesh=mesh, in_specs=in_specs, out_specs=out_specs, check_vma=False)
```
